32 devices in a mesh: dp: 8 (over z, x), fsdp: 4 (over y, core).
Axes of the slice: x: 2, y: 2, z: 4, core: 2. Of those that a mesh axis runs over, the one named last changes fastest.
Arguments:
- tokens: int32 [32768], P(('dp', 'fsdp')), may hold values from 0 to 50687
- lengths: int32 [32], P(('dp', 'fsdp')), may hold values from 256 to 1024, as said below
- loss_picks: int32 [32, 64], P(('dp', 'fsdp')), may hold values from 0 to 1048575
- embedding: bfloat16 [50688, 1024], P('fsdp'), may hold values from -0.359375 to 0.359375
- in_weight: bfloat16 [1024, 4384], P('fsdp'), may hold values from -0.1875 to 0.1875
- out_weight: bfloat16 [2048, 1024], P('fsdp'), may hold values from -0.125 to 0.125
- ahead_weight: bfloat16 [1024, 1024], P('fsdp'), may hold values from -0.1875 to 0.1875
- conv_weight: bfloat16 [5, 2304], P(None, 'fsdp'), may hold values from -3 to 3
- head_params: bfloat16 [3, 32], P(None, 'fsdp'), may hold values from -6 to 1.5, as said below
- norm_gains: bfloat16 [4096], P('fsdp'), may hold values from 0.5 to 1.5
- table_rows: float32 [50688], P('fsdp'), may hold values from 1e-16 to 5e-09
- table_columns: float32 [1024], P('dp'), may hold values from 3e-10 to 5e-09
- in_rows: float32 [1024], P('fsdp'), may hold values from 3e-10 to 5e-09
- in_columns: float32 [4384], replicated, may hold values from 3e-10 to 5e-09
- out_rows: float32 [2048], P('fsdp'), may hold values from 3e-10 to 5e-09
- out_columns: float32 [1024], replicated, may hold values from 3e-10 to 5e-09
- ahead_rows: float32 [1024], P('fsdp'), may hold values from 3e-10 to 5e-09
- ahead_columns: float32 [1024], replicated, may hold values from 3e-10 to 5e-09
- conv_moment: float32 [5, 2304], P(None, 'fsdp'), may hold values from 3e-10 to 5e-09
- head_moment: float32 [3, 32], P(None, 'fsdp'), may hold values from 3e-10 to 5e-09
- gain_moment: float32 [4096], P('fsdp'), may hold values from 3e-10 to 5e-09
Outputs:
- new_table: float32 [50688, 1024], P('fsdp', 'dp')
- new_in_weight: float32 [1024, 4384], P('fsdp')
- new_out_weight: float32 [2048, 1024], P('fsdp')
- new_ahead_weight: float32 [1024, 1024], P('fsdp')
- new_conv_weight: float32 [5, 2304], P(None, 'fsdp')
- new_head_params: float32 [3, 32], P(None, 'fsdp')
- new_norm_gains: float32 [4096], P('fsdp')
- new_table_rows: float32 [50688], P('fsdp')
- new_table_columns: float32 [1024], P('dp')
- new_in_rows: float32 [1024], P('fsdp')
- new_in_columns: float32 [4384], replicated
- new_out_rows: float32 [2048], P('fsdp')
- new_out_columns: float32 [1024], replicated
- new_ahead_rows: float32 [1024], P('fsdp')
- new_ahead_columns: float32 [1024], replicated
- new_conv_moment: float32 [5, 2304], P(None, 'fsdp')
- new_head_moment: float32 [3, 32], P(None, 'fsdp')
- new_gain_moment: float32 [4096], P('fsdp')
- loss: float32 [], replicated
- grad_norm: float32 [], replicated
The draws below stay inside these ranges and needn't reach their ends.
Inputs may be any that keep to these rules, and one draw needn't show every extreme that they name: `lengths`: some sequence has all 1024 slots valid. `head_params`: row 0 lies in -6 to -3, row 1 in -2.31 to 1.39, row 2 in 0.5 to 1.5.
All inputs are finite; a program needn't handle non-finite values.
Results may differ from the reference program's by a relative error of at most 0.0045.
Values may be sent and summed in bfloat16 or wider, within the bound.
A program may use at most 384 MiB of HBM per device.

```python
import math
import jax
import jax.numpy as jnp
import numpy as np
from jax import lax

D = 1024
HEADS = 32
HEAD_DIM = 64
STATE = 128
VOCAB = 50688
KERNEL = 4
SPAN = 256
TOK_DEV = 1024
LOSS_DEV = 64
INNER = 2048
CONV_WIDTH = 2304
IN_WIDTH = 4384
GAINS = 4096
SEQS = 32
TOKENS = 32768


def draw_lengths(key, part):
    first_key, second_key = jax.random.split(key)
    drawn_lengths = jax.random.randint(first_key, (SEQS,), TOK_DEV // 4, TOK_DEV + 1)
    chosen = jax.random.randint(second_key, (), 0, SEQS)
    return jnp.where(jnp.arange(SEQS) == chosen, TOK_DEV, drawn_lengths).astype(jnp.int32)


def draw_head_params(key, part):
    subkeys = jax.random.split(key, 3)
    step_bias = jax.random.uniform(subkeys[0], (HEADS,), jnp.float32, -6.0, -3.0)
    log_rate = jax.random.uniform(subkeys[1], (HEADS,), jnp.float32, -2.3, 1.38)
    skip_gain = jax.random.uniform(subkeys[2], (HEADS,), jnp.float32, 0.5, 1.5)
    return jnp.stack([step_bias, log_rate, skip_gain]).astype(jnp.bfloat16)


def with_ends(entries, own_key, low, top_value):
    spot = [jax.random.randint(jax.random.fold_in(own_key, axis), (), 0, length) for axis, length in enumerate(entries.shape)]
    longest = entries.shape.index(max(entries.shape))
    neighbour = spot[:longest] + [(spot[longest] + 1) % entries.shape[longest]] + spot[longest + 1:]
    return entries.at[tuple(spot)].set(low).at[tuple(neighbour)].set(top_value)


def block_levels(rng, dims, cuts, low, top_value):
    factor_of, own = 1.0, jax.random.fold_in(rng, 6)
    for position, blocks in cuts:
        heights = jnp.exp(jax.random.uniform(jax.random.fold_in(own, position), (blocks,), jnp.float32, low / len(cuts), top_value / len(cuts)))
        factor_of = factor_of * jnp.repeat(heights, dims[position] // blocks).reshape([-1 if axis == position else 1 for axis in range(len(dims))])
    return factor_of


def cumulative_ranks(amount, lean):
    portions = [(1 << 20) // math.isqrt(rank ** lean) + 1 for rank in range(1, amount + 1)]
    scale = 1 + sum(portions) // (1 << 30)
    return np.cumsum(np.array([max(1, weight // scale) for weight in portions]))


def ranked_ids(rng, extent, amount, skew):
    listing = cumulative_ranks(amount, skew)
    lot = jax.random.randint(jax.random.fold_in(rng, 1), extent, 0, int(listing[amount - 1]))
    rank = jnp.searchsorted(jnp.asarray(listing, jnp.int32), lot, side="right")
    return jax.random.permutation(jax.random.fold_in(rng, 2), amount)[rank].astype(jnp.int32)


def centred(rng, extent, scale, limit, shards=(), kind=jnp.bfloat16):
    drawn = scale * jax.random.normal(rng, extent, jnp.float32)
    if shards:
        drawn = drawn * block_levels(rng, extent, shards, -0.22, 0.18)
    return jnp.clip(drawn, -limit, limit).astype(kind)


def setup_inputs(seed: int = 0) -> dict:
    key_list = jax.random.split(jax.random.key(seed), 22)
    return {
        "tokens": with_ends(ranked_ids(key_list[0], (TOKENS,), VOCAB, 2), jax.random.fold_in(key_list[0], 3), 0, VOCAB - 1).astype(jnp.int32),
        "lengths": draw_lengths(jax.random.fold_in(key_list[21], 71), 0),
        "loss_picks": with_ends(jax.random.randint(key_list[2], (SEQS, LOSS_DEV), 0, 1048576), jax.random.fold_in(key_list[2], 1), 0, 1048575).astype(jnp.int32),
        "embedding": centred(key_list[3], (VOCAB, D), 0.06, 0.359375, ((0, 4),)),
        "in_weight": centred(key_list[4], (D, IN_WIDTH), D ** -0.5, 0.1875, ((0, 4),)),
        "out_weight": centred(key_list[5], (INNER, D), INNER ** -0.5, 0.125, ((0, 4),)),
        "ahead_weight": centred(key_list[6], (D, D), D ** -0.5, 0.1875, ((0, 4),)),
        "conv_weight": centred(key_list[7], (KERNEL + 1, CONV_WIDTH), 0.5, 3.0, ((1, 4),)),
        "head_params": draw_head_params(jax.random.fold_in(key_list[21], 71), 0),
        "norm_gains": jnp.clip(1.0 + 0.1 * jax.random.normal(key_list[9], (GAINS,), jnp.float32), 0.5, 1.5).astype(jnp.bfloat16),
        "table_rows": jnp.clip(jnp.exp(math.log(4.999999969612645e-09) - 17.727534 * jax.random.uniform(key_list[10], (VOCAB,), jnp.float32) ** block_levels(key_list[10], (VOCAB,), ((0, 4),), -0.2, 0.2)), 1.0000000168623835e-16, 4.999999969612645e-09),
        "table_columns": jnp.clip(jnp.exp(math.log(4.999999969612645e-09) - 2.8134107 * jax.random.uniform(key_list[11], (D,), jnp.float32) ** block_levels(key_list[11], (D,), ((0, 8),), -0.2, 0.2)), 2.999999970665357e-10, 4.999999969612645e-09),
        "in_rows": jnp.clip(jnp.exp(math.log(4.999999969612645e-09) - 2.8134107 * jax.random.uniform(key_list[12], (D,), jnp.float32) ** block_levels(key_list[12], (D,), ((0, 4),), -0.2, 0.2)), 2.999999970665357e-10, 4.999999969612645e-09),
        "in_columns": jnp.clip(jnp.exp(jax.random.uniform(key_list[13], (IN_WIDTH,), jnp.float32, math.log(2.999999970665357e-10), math.log(4.999999969612645e-09))), 2.999999970665357e-10, 4.999999969612645e-09),
        "out_rows": jnp.clip(jnp.exp(math.log(4.999999969612645e-09) - 2.8134107 * jax.random.uniform(key_list[14], (INNER,), jnp.float32) ** block_levels(key_list[14], (INNER,), ((0, 4),), -0.2, 0.2)), 2.999999970665357e-10, 4.999999969612645e-09),
        "out_columns": jnp.clip(jnp.exp(jax.random.uniform(key_list[15], (D,), jnp.float32, math.log(2.999999970665357e-10), math.log(4.999999969612645e-09))), 2.999999970665357e-10, 4.999999969612645e-09),
        "ahead_rows": jnp.clip(jnp.exp(math.log(4.999999969612645e-09) - 2.8134107 * jax.random.uniform(key_list[16], (D,), jnp.float32) ** block_levels(key_list[16], (D,), ((0, 4),), -0.2, 0.2)), 2.999999970665357e-10, 4.999999969612645e-09),
        "ahead_columns": jnp.clip(jnp.exp(jax.random.uniform(key_list[17], (D,), jnp.float32, math.log(2.999999970665357e-10), math.log(4.999999969612645e-09))), 2.999999970665357e-10, 4.999999969612645e-09),
        "conv_moment": jnp.clip(jnp.exp(math.log(4.999999969612645e-09) - 2.8134107 * jax.random.uniform(key_list[18], (KERNEL + 1, CONV_WIDTH), jnp.float32) ** block_levels(key_list[18], (KERNEL + 1, CONV_WIDTH), ((1, 4),), -0.2, 0.2)), 2.999999970665357e-10, 4.999999969612645e-09),
        "head_moment": jnp.clip(jnp.exp(math.log(4.999999969612645e-09) - 2.8134107 * jax.random.uniform(key_list[19], (3, HEADS), jnp.float32) ** block_levels(key_list[19], (3, HEADS), ((1, 4),), -0.2, 0.2)), 2.999999970665357e-10, 4.999999969612645e-09),
        "gain_moment": jnp.clip(jnp.exp(math.log(4.999999969612645e-09) - 2.8134107 * jax.random.uniform(key_list[20], (GAINS,), jnp.float32) ** block_levels(key_list[20], (GAINS,), ((0, 4),), -0.2, 0.2)), 2.999999970665357e-10, 4.999999969612645e-09),
    }


PRECISE = lax.Precision.HIGHEST
EPSILON = 1e-05
DECAY_RATE = 0.5
STEP_RATE = 0.2
CLIP_NORM = 0.2
AFTER_SHARE = 0.3
FLOOR_RMS = 0.001
MASK_FILL = -10000.0

@jax.custom_vjp
def low(v):
    return lax.optimization_barrier(v.astype(jnp.bfloat16)).astype(jnp.float32)

@jax.custom_vjp
def low_back(v):
    return v

def low_keep(v):
    return (low(v), None)

def low_pass(kept, grad):
    return (grad,)

def back_keep(v):
    return (v, None)

def back_low(kept, grad):
    return (low(grad),)
low.defvjp(low_keep, low_pass)
low_back.defvjp(back_keep, back_low)

def rms_norm(values_in, gain_in):
    return values_in * lax.rsqrt(lax.optimization_barrier(jnp.mean(values_in * values_in, axis=-1, keepdims=True)) + EPSILON) * gain_in

def block_step(carried, pieces):
    block_x, block_steps, block_rates, block_keys, block_queries = pieces
    log_decay = jnp.cumsum(block_rates, axis=0)
    row_index = jnp.arange(block_rates.shape[0])
    causal = row_index[:, None] >= row_index[None, :]
    decay_grid = jnp.exp(jnp.where(causal[:, :, None], log_decay[:, None, :] - log_decay[None, :, :], MASK_FILL))
    scores = jnp.dot(block_queries, block_keys.T, precision=PRECISE)
    mix_weights = scores[:, :, None] * decay_grid * block_steps[None, :, :]
    within = jnp.einsum('tsh,shp->thp', mix_weights, block_x, precision=PRECISE)
    from_state = jnp.exp(log_decay)[:, :, None] * jnp.einsum('tn,hpn->thp', block_queries, carried, precision=PRECISE)
    tail_decay = jnp.exp(log_decay[-1][None, :] - log_decay) * block_steps
    carried = jnp.exp(log_decay[-1])[:, None, None] * carried + jnp.einsum('sh,shp,sn->hpn', tail_decay, block_x, block_keys, precision=PRECISE)
    return (carried, within + from_state)

def state_mixer(projected, conv_table, head_table, gain_in):
    length = projected.shape[0]
    gate_part = projected[:, :INNER]
    conv_input = projected[:, INNER:INNER + CONV_WIDTH]
    step_raw = projected[:, INNER + CONV_WIDTH:]
    padded = jnp.concatenate([jnp.zeros((KERNEL - 1, CONV_WIDTH), jnp.float32), conv_input], axis=0)
    conv_sum = conv_table[KERNEL]
    for offset in range(KERNEL):
        conv_sum = conv_sum + conv_table[offset] * padded[offset:offset + length]
    activated = jax.nn.silu(conv_sum)
    x_heads = activated[:, :INNER].reshape(length, HEADS, HEAD_DIM)
    key_part = activated[:, INNER:INNER + STATE]
    query_part = activated[:, INNER + STATE:]
    step_size = jax.nn.softplus(step_raw + head_table[0])
    rates = -step_size * jnp.exp(head_table[1])
    blocks = length // SPAN
    initial = jnp.zeros((HEADS, HEAD_DIM, STATE), jnp.float32)
    _, head_out = lax.scan(jax.checkpoint(block_step), initial, (x_heads.reshape(blocks, SPAN, HEADS, HEAD_DIM), step_size.reshape(blocks, SPAN, HEADS), rates.reshape(blocks, SPAN, HEADS), key_part.reshape(blocks, SPAN, STATE), query_part.reshape(blocks, SPAN, STATE)))
    head_out = head_out.reshape(length, HEADS, HEAD_DIM) + head_table[2][None, :, None] * x_heads
    gated = head_out.reshape(length, INNER) * jax.nn.silu(gate_part)
    return rms_norm(gated, gain_in)

def layer_rows(embedded, place_row, in_matrix, out_matrix, conv_table, head_table, gain_table):
    normed = low(rms_norm(embedded, gain_table[:D]))
    projected = low_back(jnp.dot(normed, in_matrix, precision=PRECISE))
    mixed = low(state_mixer(projected, conv_table, head_table, gain_table[D + D:]))
    residual = embedded + low_back(jnp.dot(mixed, out_matrix, precision=PRECISE))
    final_norm = rms_norm(residual, gain_table[D:D + D])
    return final_norm[place_row]

def cross_entropy(rows_in, targets, vocab_table):
    logits = low_back(jnp.dot(rows_in, vocab_table.T, precision=PRECISE))
    row_max = lax.optimization_barrier(jnp.max(logits, axis=1, keepdims=True))
    spread = jnp.log(lax.optimization_barrier(jnp.sum(jnp.exp(logits - row_max), axis=1))) + row_max[:, 0]
    picked = jnp.take_along_axis(logits, targets[:, None], axis=1)[:, 0]
    return jnp.sum(spread - picked)

def forward(weights, token_grid, places, next_ids, after_ids):
    vocab_table, in_matrix, out_matrix, ahead_matrix, conv_table, head_table, gain_table = weights
    embedded = vocab_table[token_grid]

    def one_sequence(member):
        return layer_rows(member[0], member[1], in_matrix, out_matrix, conv_table, head_table, gain_table)
    picked_rows = lax.map(jax.checkpoint(one_sequence), (embedded, places))
    first_rows = low(picked_rows.reshape(-1, D))
    second_rows = low_back(low(jnp.dot(first_rows, ahead_matrix, precision=PRECISE)))
    total_rows = first_rows.shape[0]
    block_rows = min(512, total_rows)
    count_blocks = total_rows // block_rows

    def block_loss(member):
        return cross_entropy(member[0], member[2], vocab_table) + AFTER_SHARE * cross_entropy(member[1], member[3], vocab_table)
    block_losses = lax.map(jax.checkpoint(block_loss), (first_rows.reshape(count_blocks, block_rows, D), second_rows.reshape(count_blocks, block_rows, D), next_ids.reshape(count_blocks, block_rows), after_ids.reshape(count_blocks, block_rows)))
    return jnp.sum(block_losses) / total_rows

def factored(weight, gradient, rows_old, columns_old):
    squared = gradient * gradient
    rows_new = DECAY_RATE * rows_old + (1.0 - DECAY_RATE) * lax.optimization_barrier(jnp.mean(squared, axis=1))
    columns_new = DECAY_RATE * columns_old + (1.0 - DECAY_RATE) * lax.optimization_barrier(jnp.mean(squared, axis=0))
    estimate = rows_new[:, None] * columns_new[None, :] / jnp.mean(rows_new)
    step_size = STEP_RATE * jnp.maximum(FLOOR_RMS, jnp.sqrt(jnp.mean(weight * weight)))
    return (weight - step_size * gradient * lax.rsqrt(estimate), rows_new, columns_new)

def unfactored(weight, gradient, moment_old):
    moment_new = DECAY_RATE * moment_old + (1.0 - DECAY_RATE) * gradient * gradient
    step_size = STEP_RATE * jnp.maximum(FLOOR_RMS, jnp.sqrt(jnp.mean(weight * weight)))
    return (weight - step_size * gradient * lax.rsqrt(moment_new), moment_new)

def reference(tokens, lengths, loss_picks, embedding, in_weight, out_weight, ahead_weight, conv_weight, head_params, norm_gains, table_rows, table_columns, in_rows, in_columns, out_rows, out_columns, ahead_rows, ahead_columns, conv_moment, head_moment, gain_moment):
    seq_count = lengths.shape[0]
    token_grid = tokens.reshape(seq_count, TOK_DEV)
    places = (loss_picks % (lengths[:, None] - 2)).astype(jnp.int32)
    seq_index = jnp.arange(seq_count, dtype=jnp.int32)[:, None]
    next_ids = token_grid[seq_index, places + 1].reshape(-1)
    after_ids = token_grid[seq_index, places + 2].reshape(-1)
    weights = tuple((weight.astype(jnp.float32) for weight in (embedding, in_weight, out_weight, ahead_weight, conv_weight, head_params, norm_gains)))

    def loss_of(*params):
        return forward(params, token_grid, places, next_ids, after_ids)
    loss, pullback = jax.vjp(loss_of, *weights)
    gradients = pullback(jnp.ones((), jnp.float32))
    grad_norm = jnp.sqrt(sum((jnp.sum(gradient * gradient) for gradient in gradients)))
    factor = jnp.minimum(1.0, CLIP_NORM / grad_norm)
    clipped = [gradient * factor for gradient in gradients]
    new_table, new_table_rows, new_table_columns = factored(weights[0], clipped[0], table_rows, table_columns)
    new_in, new_in_rows, new_in_columns = factored(weights[1], clipped[1], in_rows, in_columns)
    new_out, new_out_rows, new_out_columns = factored(weights[2], clipped[2], out_rows, out_columns)
    new_ahead, new_ahead_rows, new_ahead_columns = factored(weights[3], clipped[3], ahead_rows, ahead_columns)
    new_conv, new_conv_moment = unfactored(weights[4], clipped[4], conv_moment)
    new_heads, new_head_moment = unfactored(weights[5], clipped[5], head_moment)
    new_gains, new_gain_moment = unfactored(weights[6], clipped[6], gain_moment)
    return (new_table, new_in, new_out, new_ahead, new_conv, new_heads, new_gains, new_table_rows, new_table_columns, new_in_rows, new_in_columns, new_out_rows, new_out_columns, new_ahead_rows, new_ahead_columns, new_conv_moment, new_head_moment, new_gain_moment, loss, grad_norm)
```

```python
import jax
import jax.numpy as jnp
from jax import lax
from jax.experimental import pallas as pl
from jax.experimental.pallas import tpu as pltpu
from jax.sharding import PartitionSpec as P

D = 1024
HEADS = 32
HEAD_DIM = 64
STATE = 128
VOCAB = 50688
KERNEL = 4
SPAN = 256
INNER = 2048
CONV_WIDTH = 2304
IN_WIDTH = 4384
GAINS = 4096
GROUP = 4
PAD = 8
CHUNK = 128


PRECISE = lax.Precision.HIGHEST
EPSILON = 1e-05
DECAY_RATE = 0.5
STEP_RATE = 0.2
CLIP_NORM = 0.2
AFTER_SHARE = 0.3
FLOOR_RMS = 0.001
MASK_FILL = -10000.0


def merged_2(value, axis, join):
    pieces = jax.tree.map(lambda part: lax.all_gather(part, axis), value)
    head = jax.tree.map(lambda part: part[0], pieces)
    tail = jax.tree.map(lambda part: part[1:], pieces)
    running, _ = lax.scan(lambda running, piece: (join(running, piece), None), head, tail)
    return running


def rms_norm(values_in, gain_in):
    return (
        values_in
        * lax.rsqrt(jnp.mean(values_in * values_in, axis=-1, keepdims=True) + EPSILON)
        * gain_in
    )


def gated_norm(head_rows, gate_rows, gain_in):
    return rms_norm(head_rows * jax.nn.silu(gate_rows), gain_in)


def contract(one_side, other_side, one_dim, other_dim):
    return lax.dot_general(
        one_side,
        other_side,
        (((one_dim,), (other_dim,)), ((), ())),
        preferred_element_type=jnp.float32,
    )


def split(value):
    high = value.astype(jnp.bfloat16)
    return high, (value - high.astype(jnp.float32)).astype(jnp.bfloat16)


def product(one_side, other_side, one_dim, other_dim):
    return lax.dot_general(
        one_side,
        other_side,
        (((one_dim,), (other_dim,)), ((), ())),
        preferred_element_type=jnp.float32,
    )


def product_3(one_side, other_side, one_dim, other_dim):
    one_high, one_low = one_side
    other_high, other_low = other_side
    return (
        product(one_high, other_high, one_dim, other_dim)
        + product(one_low, other_high, one_dim, other_dim)
        + product(one_high, other_low, one_dim, other_dim)
    )


def exact(one_side, other_side, one_dim, other_dim):
    return lax.dot_general(
        one_side,
        other_side,
        (((one_dim,), (other_dim,)), ((), ())),
        precision=PRECISE,
        preferred_element_type=jnp.float32,
    )


def running_sum(values, backward):
    length = values.shape[1]
    lane = lax.broadcasted_iota(jnp.int32, values.shape, 1)
    shift = 1
    while shift < length:
        if backward:
            moved = pltpu.roll(values, length - shift, 1)
            values = values + jnp.where(lane < length - shift, moved, 0.0)
        else:
            moved = pltpu.roll(values, shift, 1)
            values = values + jnp.where(lane >= shift, moved, 0.0)
        shift *= 2
    return values


def taps_sum(window, taps_ref, rows):
    total = taps_ref[KERNEL : KERNEL + 1, :]
    for offset in range(KERNEL):
        start = PAD - KERNEL + 1 + offset
        total = total + taps_ref[offset : offset + 1, :] * window[start : start + rows]
    return total


def sigmoid(value):
    return 1.0 / (1.0 + jnp.exp(-value))


def decay_spread(row_decay, places, lane):
    here = lane == places
    at_place = jnp.sum(jnp.where(here, row_decay, 0.0), axis=1, keepdims=True)
    return jnp.exp(jnp.where(lane <= places, at_place - row_decay, MASK_FILL)), here


def mix_forward_kernel(
    normed_ref,
    weight_ref,
    taps_ref,
    raw_ref,
    columns_ref,
    places_ref,
    skip_ref,
    input_ref,
    out_ref,
    scores_ref,
    keys_ref,
    queries_ref,
    steps_ref,
    decay_ref,
    padded,
    active,
    mix_high,
    mix_low,
):
    step = pl.program_id(0)
    length = normed_ref.shape[0]
    rows = places_ref.shape[0]
    width = weight_ref.shape[1]
    chunk = CHUNK
    places = places_ref[...]
    lane = lax.broadcasted_iota(jnp.int32, (rows, length), 1)
    value = product(normed_ref[...], weight_ref[...], 1, 0)
    input_ref[...] = value
    padded[0:PAD, :] = jnp.zeros((PAD, width), jnp.float32)
    padded[PAD:, :] = value

    def activate(index, carry):
        start = pl.multiple_of(index * chunk, chunk)
        window = padded[pl.ds(start, chunk + PAD), :]
        total = taps_sum(window, taps_ref, chunk)
        active[pl.ds(start, chunk), :] = total * sigmoid(total)
        return carry

    lax.fori_loop(0, length // chunk, activate, 0)

    @pl.when(step == 0)
    def _():
        keys = active[:, :STATE]
        keys_ref[...] = keys
        picked = exact((lane == places).astype(jnp.float32), active[:, STATE:], 1, 0)
        queries_ref[...] = picked
        scores_ref[...] = exact(picked, keys, 1, 1)
        shifted = raw_ref[...] + columns_ref[:, 0:1]
        steps = jnp.maximum(shifted, 0.0) + jnp.log1p(jnp.exp(-jnp.abs(shifted)))
        steps_ref[...] = steps
        decay_ref[...] = running_sum(-steps * jnp.exp(columns_ref[:, 1:2]), False)

    @pl.when(step > 0)
    def _():
        scores = scores_ref[...]
        for index in range(GROUP):
            head = (step - 1) * GROUP + index
            row_steps = steps_ref[pl.ds(head, 1), :]
            spread, here = decay_spread(decay_ref[pl.ds(head, 1), :], places, lane)
            weights = scores * spread * row_steps + jnp.where(here, skip_ref[head], 0.0)
            high, low = split(weights)
            mix_high[index * rows : (index + 1) * rows, :] = high
            mix_low[index * rows : (index + 1) * rows, :] = low
        x_pair = split(active[...])
        mixed = product_3((mix_high[...], mix_low[...]), x_pair, 1, 0)
        column = lax.broadcasted_iota(jnp.int32, (rows, width), 1) // HEAD_DIM
        total = jnp.zeros((rows, width), jnp.float32)
        for index in range(GROUP):
            total = jnp.where(column == index, mixed[index * rows : (index + 1) * rows], total)
        out_ref[...] = total


def mix_forward(normed, weight, taps, raw, columns, places, skip):
    length = normed.shape[0]
    rows = places.shape[0]
    width = GROUP * HEAD_DIM
    blocks = CONV_WIDTH // width
    last = blocks - 1
    whole = lambda shape: pl.BlockSpec(shape, lambda step: (0,) * len(shape))
    turned = lambda step: (0, lax.rem(step + last, blocks))
    f32 = jnp.float32
    return pl.pallas_call(
        mix_forward_kernel,
        grid=(blocks,),
        in_specs=[
            whole((length, D)),
            pl.BlockSpec((D, width), turned),
            pl.BlockSpec((KERNEL + 1, width), turned),
            whole((HEADS, length)),
            whole((HEADS, 3)),
            whole((rows, 1)),
            pl.BlockSpec(memory_space=pltpu.SMEM),
        ],
        out_specs=[
            pl.BlockSpec((length, width), turned),
            pl.BlockSpec((rows, width), lambda step: (0, jnp.maximum(step - 1, 0))),
            whole((rows, length)),
            whole((length, STATE)),
            whole((rows, STATE)),
            whole((HEADS, length)),
            whole((HEADS, length)),
        ],
        out_shape=[
            jax.ShapeDtypeStruct((length, CONV_WIDTH), f32),
            jax.ShapeDtypeStruct((rows, INNER), f32),
            jax.ShapeDtypeStruct((rows, length), f32),
            jax.ShapeDtypeStruct((length, STATE), f32),
            jax.ShapeDtypeStruct((rows, STATE), f32),
            jax.ShapeDtypeStruct((HEADS, length), f32),
            jax.ShapeDtypeStruct((HEADS, length), f32),
        ],
        scratch_shapes=[
            pltpu.VMEM((length + PAD, width), f32),
            pltpu.VMEM((length, width), f32),
            pltpu.VMEM((GROUP * rows, length), jnp.bfloat16),
            pltpu.VMEM((GROUP * rows, length), jnp.bfloat16),
        ],
        compiler_params=pltpu.CompilerParams(vmem_limit_bytes=40 << 20),
        cost_estimate=pl.CostEstimate(
            flops=2 * length * D * CONV_WIDTH * 2,
            bytes_accessed=16 << 20,
            transcendentals=HEADS * rows * length,
        ),
        name="mix_forward",
    )(normed, weight, taps, raw, columns, places, skip)


def mix_backward_kernel(
    input_ref,
    taps_ref,
    grad_ref,
    scores_ref,
    keys_ref,
    queries_ref,
    steps_ref,
    decay_ref,
    raw_ref,
    columns_ref,
    places_ref,
    skip_ref,
    d_input_ref,
    d_taps_ref,
    d_raw_ref,
    d_columns_ref,
    padded,
    active,
    d_active,
    d_padded,
    mix_high,
    mix_low,
    d_mix,
    d_scores,
    d_steps,
    from_place,
    d_skip,
):
    step = pl.program_id(0)
    last = pl.num_programs(0) - 1
    length, width = input_ref.shape
    rows = places_ref.shape[0]
    chunk = CHUNK
    count = length // chunk
    places = places_ref[...]
    lane = lax.broadcasted_iota(jnp.int32, (rows, length), 1)
    padded[0:PAD, :] = jnp.zeros((PAD, width), jnp.float32)
    padded[PAD:, :] = input_ref[...]

    @pl.when(step == 0)
    def _():
        d_scores[...] = jnp.zeros_like(d_scores)

    @pl.when(step < last)
    def _():
        def activate(index, carry):
            start = pl.multiple_of(index * chunk, chunk)
            window = padded[pl.ds(start, chunk + PAD), :]
            total = taps_sum(window, taps_ref, chunk)
            active[pl.ds(start, chunk), :] = total * sigmoid(total)
            return carry

        lax.fori_loop(0, count, activate, 0)
        x_pair = split(active[...])
        column = lax.broadcasted_iota(jnp.int32, (rows, width), 1) // HEAD_DIM
        grad = grad_ref[...]
        stacked = split(
            jnp.concatenate(
                [jnp.where(column == index, grad, 0.0) for index in range(GROUP)], axis=0
            )
        )
        d_mix[...] = product_3(stacked, x_pair, 1, 1)
        scores = scores_ref[...]
        for index in range(GROUP):
            head = step * GROUP + index
            row_steps = steps_ref[pl.ds(head, 1), :]
            spread, here = decay_spread(decay_ref[pl.ds(head, 1), :], places, lane)
            weights = scores * spread
            part = d_mix[index * rows : (index + 1) * rows, :]
            d_scores[...] += part * spread * row_steps
            shared = part * weights
            d_steps[pl.ds(head, 1), :] = jnp.sum(shared, axis=0, keepdims=True)
            row_total = jnp.sum(shared * row_steps, axis=1, keepdims=True)
            from_place[pl.ds(head, 1), :] = jnp.sum(
                jnp.where(lane <= places, row_total, 0.0), axis=0, keepdims=True
            )
            d_skip[pl.ds(head, 1), :] = jnp.sum(
                jnp.where(here, part, 0.0), axis=0, keepdims=True
            )
            full = weights * row_steps + jnp.where(here, skip_ref[head], 0.0)
            high, low = split(full)
            mix_high[index * rows : (index + 1) * rows, :] = high
            mix_low[index * rows : (index + 1) * rows, :] = low
        d_active[...] = product_3((mix_high[...], mix_low[...]), stacked, 0, 0)

    @pl.when(step == last)
    def _():
        onehot = (lane == places).astype(jnp.float32)
        d_score = d_scores[...]
        d_queries = exact(d_score, keys_ref[...], 1, 0)
        d_active[:, :STATE] = exact(d_score, queries_ref[...], 0, 0)
        d_active[:, STATE:] = exact(onehot, d_queries, 0, 0)
        steps = steps_ref[...]
        direct = d_steps[...]
        rates_scale = -jnp.exp(columns_ref[:, 1:2])
        d_rates = from_place[...] - running_sum(direct * steps, True)
        d_step = direct + d_rates * rates_scale
        d_raw = d_step * sigmoid(raw_ref[...] + columns_ref[:, 0:1])
        d_raw_ref[...] = d_raw
        d_log = jnp.sum(d_rates * steps, axis=1, keepdims=True) * rates_scale
        slot = lax.broadcasted_iota(jnp.int32, d_columns_ref.shape, 1)
        d_columns_ref[...] = jnp.where(
            slot == 0,
            jnp.sum(d_raw, axis=1, keepdims=True),
            jnp.where(slot == 1, d_log, jnp.sum(d_skip[...], axis=1, keepdims=True)),
        )

    d_padded[length:, :] = jnp.zeros((PAD, width), jnp.float32)

    def through_silu(index, carry):
        start = pl.multiple_of(index * chunk, chunk)
        window = padded[pl.ds(start, chunk + PAD), :]
        total = taps_sum(window, taps_ref, chunk)
        gate = sigmoid(total)
        d_total = d_active[pl.ds(start, chunk), :] * (gate * (1.0 + total * (1.0 - gate)))
        d_padded[pl.ds(start, chunk), :] = d_total
        sums = []
        for offset in range(KERNEL):
            begin = PAD - KERNEL + 1 + offset
            sums.append(jnp.sum(d_total * window[begin : begin + chunk], axis=0, keepdims=True))
        sums.append(jnp.sum(d_total, axis=0, keepdims=True))
        return tuple(one + other for one, other in zip(carry, sums))

    sums = lax.fori_loop(
        0, count, through_silu, tuple(jnp.zeros((1, width), jnp.float32) for _ in range(KERNEL + 1))
    )
    for offset in range(KERNEL + 1):
        d_taps_ref[offset : offset + 1, :] = sums[offset]

    def through_taps(index, carry):
        start = pl.multiple_of(index * chunk, chunk)
        window = d_padded[pl.ds(start, chunk + PAD), :]
        total = taps_ref[KERNEL - 1 : KERNEL, :] * window[:chunk]
        for offset in range(KERNEL - 1):
            begin = KERNEL - 1 - offset
            total = total + taps_ref[offset : offset + 1, :] * window[begin : begin + chunk]
        d_input_ref[pl.ds(start, chunk), :] = total.astype(d_input_ref.dtype)
        return carry

    lax.fori_loop(0, count, through_taps, 0)


def mix_backward(inputs, taps, grad, scores, keys, queries, steps, decay, raw, columns, places, skip):
    length = inputs.shape[0]
    rows = places.shape[0]
    width = GROUP * HEAD_DIM
    blocks = CONV_WIDTH // width
    whole = lambda shape: pl.BlockSpec(shape, lambda step: (0,) * len(shape))
    along = lambda step: (0, step)
    f32 = jnp.float32
    return pl.pallas_call(
        mix_backward_kernel,
        grid=(blocks,),
        in_specs=[
            pl.BlockSpec((length, width), along),
            pl.BlockSpec((KERNEL + 1, width), along),
            pl.BlockSpec((rows, width), lambda step: (0, jnp.minimum(step, blocks - 2))),
            whole((rows, length)),
            whole((length, STATE)),
            whole((rows, STATE)),
            whole((HEADS, length)),
            whole((HEADS, length)),
            whole((HEADS, length)),
            whole((HEADS, 3)),
            whole((rows, 1)),
            pl.BlockSpec(memory_space=pltpu.SMEM),
        ],
        out_specs=[
            pl.BlockSpec((length, width), along),
            pl.BlockSpec((KERNEL + 1, width), along),
            whole((HEADS, length)),
            whole((HEADS, 128)),
        ],
        out_shape=[
            jax.ShapeDtypeStruct((length, CONV_WIDTH), jnp.bfloat16),
            jax.ShapeDtypeStruct((KERNEL + 1, CONV_WIDTH), f32),
            jax.ShapeDtypeStruct((HEADS, length), f32),
            jax.ShapeDtypeStruct((HEADS, 128), f32),
        ],
        scratch_shapes=[
            pltpu.VMEM((length + PAD, width), f32),
            pltpu.VMEM((length, width), f32),
            pltpu.VMEM((length, width), f32),
            pltpu.VMEM((length + PAD, width), f32),
            pltpu.VMEM((GROUP * rows, length), jnp.bfloat16),
            pltpu.VMEM((GROUP * rows, length), jnp.bfloat16),
            pltpu.VMEM((GROUP * rows, length), f32),
            pltpu.VMEM((rows, length), f32),
            pltpu.VMEM((HEADS, length), f32),
            pltpu.VMEM((HEADS, length), f32),
            pltpu.VMEM((HEADS, length), f32),
        ],
        compiler_params=pltpu.CompilerParams(vmem_limit_bytes=48 << 20),
        cost_estimate=pl.CostEstimate(
            flops=6 * HEADS * rows * length * HEAD_DIM * 4,
            bytes_accessed=20 << 20,
            transcendentals=HEADS * rows * length,
        ),
        name="mix_backward",
    )(inputs, taps, grad, scores, keys, queries, steps, decay, raw, columns, places, skip)


def shard_terms(logits, local_target):
    row_max = jnp.max(logits, axis=1)
    exp_total = jnp.sum(jnp.exp(logits - row_max[:, None]), axis=1)
    onehot = (jnp.arange(logits.shape[1])[None, :] == local_target[:, None]).astype(jnp.float32)
    picked = jnp.sum(onehot * logits, axis=1)
    return (row_max, exp_total, picked, onehot)


def combine_totals(one_side, other_side):
    combined = []
    for base in (0, 3):
        row_max = jnp.maximum(one_side[base], other_side[base])
        exp_total = one_side[base + 1] * jnp.exp(one_side[base] - row_max) + other_side[
            base + 1
        ] * jnp.exp(other_side[base] - row_max)
        combined = combined + [row_max, exp_total, one_side[base + 2] + other_side[base + 2]]
    return tuple(combined)


def shards(
    tokens,
    lengths,
    loss_picks,
    embedding,
    in_weight,
    out_weight,
    ahead_weight,
    conv_weight,
    head_params,
    norm_gains,
    table_rows,
    table_columns,
    in_rows,
    in_columns,
    out_rows,
    out_columns,
    ahead_rows,
    ahead_columns,
    conv_moment,
    head_moment,
    gain_moment,
):
    group_size = lax.axis_size("fsdp")
    my_rank = lax.axis_index("fsdp")
    replica_count = lax.axis_size("dp")
    replica_rank = lax.axis_index("dp")
    seq_len = tokens.shape[0]
    places = loss_picks[0] % (lengths[0] - 2)
    loss_rows = places.shape[0]
    packed = jnp.concatenate([tokens, tokens[places + 1], tokens[places + 2]])
    group_ids = lax.all_gather(packed, "fsdp", axis=0, tiled=True).reshape(
        group_size, seq_len + 2 * loss_rows
    )
    all_tokens = group_ids[:, :seq_len].reshape(-1)
    next_ids = group_ids[:, seq_len : seq_len + loss_rows].reshape(-1)
    after_ids = group_ids[:, seq_len + loss_rows :].reshape(-1)
    vocab_part = embedding.shape[0]
    width_total = embedding.shape[1]
    column_part = width_total // replica_count
    first_id = my_rank * vocab_part
    local_ids = all_tokens - first_id
    inside = (local_ids >= 0) & (local_ids < vocab_part)
    safe_ids = jnp.clip(local_ids, 0, vocab_part - 1)
    looked = jnp.where(inside[:, None], embedding[safe_ids], jnp.zeros((), jnp.bfloat16)).astype(
        jnp.float32
    )
    embedded = lax.psum_scatter(
        looked.astype(jnp.bfloat16), "fsdp", scatter_dimension=0, tiled=True
    ).astype(jnp.float32)
    in_gate, in_conv, in_step, out_matrix, ahead_matrix, conv_table, head_table, gain_table = (
        lax.all_gather(in_weight[:, :INNER], "fsdp", axis=0, tiled=True),
        lax.all_gather(in_weight[:, INNER : INNER + CONV_WIDTH], "fsdp", axis=0, tiled=True),
        lax.all_gather(in_weight[:, INNER + CONV_WIDTH :], "fsdp", axis=0, tiled=True),
        lax.all_gather(out_weight, "fsdp", axis=0, tiled=True),
        lax.all_gather(ahead_weight, "fsdp", axis=0, tiled=True),
        lax.all_gather(conv_weight, "fsdp", axis=1, tiled=True).astype(jnp.float32),
        lax.all_gather(head_params, "fsdp", axis=1, tiled=True).astype(jnp.float32),
        lax.all_gather(norm_gains, "fsdp", axis=0, tiled=True).astype(jnp.float32),
    )
    normed, pull_pre = jax.vjp(rms_norm, embedded, gain_table[:D])
    normed_low = normed.astype(jnp.bfloat16)
    raw = contract(in_step, normed_low, 0, 1)
    columns = head_table.T
    place_column = places[:, None]
    inputs, head_rows, scores, keys, queries, steps, decay = mix_forward(
        normed_low, in_conv, conv_table, raw, columns, place_column, head_table[2]
    )
    embedded_rows = embedded[places]
    normed_rows, pull_rows = jax.vjp(rms_norm, embedded_rows, gain_table[:D])
    normed_rows = normed_rows.astype(jnp.bfloat16)
    gate_rows = contract(normed_rows, in_gate, 1, 0)
    mixed, pull_mix = jax.vjp(gated_norm, head_rows, gate_rows, gain_table[D + D :])
    mixed_low = mixed.astype(jnp.bfloat16)
    residual = embedded_rows + contract(mixed_low, out_matrix, 1, 0)
    final_norm, pull_final = jax.vjp(rms_norm, residual, gain_table[D : D + D])
    first_low = final_norm.astype(jnp.bfloat16)
    second_low = jnp.dot(first_low, ahead_matrix, preferred_element_type=jnp.float32).astype(
        jnp.bfloat16
    )
    group_first, group_second = (
        lax.all_gather(first_low, "fsdp", axis=0, tiled=True),
        lax.all_gather(second_low, "fsdp", axis=0, tiled=True),
    )
    logits_next = contract(group_first, embedding, 1, 1)
    logits_after = contract(group_second, embedding, 1, 1)
    max_next, sum_next, pick_next, hot_next = shard_terms(logits_next, next_ids - first_id)
    max_after, sum_after, pick_after, hot_after = shard_terms(logits_after, after_ids - first_id)
    merged = merged_2(
        (max_next, sum_next, pick_next, max_after, sum_after, pick_after), "fsdp", combine_totals
    )
    lse_next = merged[0] + jnp.log(merged[1])
    lse_after = merged[3] + jnp.log(merged[4])
    count_all = loss_rows * group_size * replica_count
    group_loss = (
        jnp.sum(lse_next - merged[2]) + AFTER_SHARE * jnp.sum(lse_after - merged[5])
    ) / count_all
    grad_next = ((jnp.exp(logits_next - lse_next[:, None]) - hot_next) / count_all).astype(
        jnp.bfloat16
    )
    grad_after = (
        (jnp.exp(logits_after - lse_after[:, None]) - hot_after) * (AFTER_SHARE / count_all)
    ).astype(jnp.bfloat16)
    rows_next_grad = contract(grad_next, embedding, 1, 0)
    rows_after_grad = contract(grad_after, embedding, 1, 0)
    d_first_own, d_second_own = (
        lax.psum_scatter(rows_next_grad, "fsdp", scatter_dimension=0, tiled=True),
        lax.psum_scatter(rows_after_grad, "fsdp", scatter_dimension=0, tiled=True),
    )
    d_second = d_second_own.astype(jnp.bfloat16)
    d_ahead = contract(first_low, d_second, 0, 0)
    d_first = d_first_own + contract(d_second, ahead_matrix, 1, 1)
    d_residual, d_gain_final = pull_final(d_first)
    d_out = d_residual.astype(jnp.bfloat16)
    d_out_weight = contract(mixed_low, d_out, 0, 0)
    d_mixed = contract(d_out, out_matrix, 1, 1)
    d_head_rows, d_gate, d_gain_mix = pull_mix(d_mixed)
    d_gate_low = d_gate.astype(jnp.bfloat16)
    d_in_gate = contract(normed_rows, d_gate_low, 0, 0)
    d_pre_rows, d_gain_rows = pull_rows(contract(d_gate_low, in_gate, 1, 1))
    d_inputs, d_conv, d_raw, d_columns = mix_backward(
        inputs,
        conv_table,
        d_head_rows,
        scores,
        keys,
        queries,
        steps,
        decay,
        raw,
        columns,
        place_column,
        head_table[2],
    )
    d_heads = d_columns[:, :3].T
    d_raw_low = d_raw.astype(jnp.bfloat16)
    d_in_conv = contract(normed_low, d_inputs, 0, 0)
    d_in_step = contract(normed_low, d_raw_low, 0, 1)
    d_normed = contract(d_inputs, in_conv, 1, 1) + contract(d_raw_low, in_step, 0, 1)
    d_pre, d_gain_first = pull_pre(d_normed)
    d_gain_first = d_gain_first + d_gain_rows
    onehot = (lax.broadcasted_iota(jnp.int32, (seq_len, loss_rows), 0) == places[None, :]).astype(
        jnp.float32
    )
    d_embedded = d_pre + jnp.dot(onehot, d_residual + d_pre_rows, precision=PRECISE)
    d_in_weight = jnp.concatenate([d_in_gate, d_in_conv, d_in_step], axis=1)
    group_grads = lax.all_gather(
        d_embedded.astype(jnp.bfloat16), "fsdp", axis=0, tiled=True
    ).astype(d_embedded.dtype)
    masked_grads = jnp.where(inside[:, None], group_grads, 0.0)
    d_gains = jnp.concatenate([d_gain_first, d_gain_final, d_gain_mix])
    shares = (
        lax.psum_scatter(d_in_weight, "fsdp", scatter_dimension=0, tiled=True),
        lax.psum_scatter(d_out_weight, "fsdp", scatter_dimension=0, tiled=True),
        lax.psum_scatter(d_ahead, "fsdp", scatter_dimension=0, tiled=True),
        lax.psum_scatter(d_conv, "fsdp", scatter_dimension=1, tiled=True),
        lax.psum_scatter(d_heads, "fsdp", scatter_dimension=1, tiled=True),
        lax.psum_scatter(d_gains, "fsdp", scatter_dimension=0, tiled=True),
    )
    d_table = contract(grad_next, group_first, 0, 0) + contract(grad_after, group_second, 0, 0)
    d_table = d_table.at[safe_ids].add(masked_grads)
    table_own = lax.psum_scatter(
        d_table.astype(jnp.bfloat16), "dp", scatter_dimension=1, tiled=True
    ).astype(jnp.float32)
    summed = lax.psum(
        (shares[0], shares[1], shares[2], shares[3], shares[4], shares[5], group_loss), "dp"
    )
    gradients = [table_own] + list(summed[:6])
    loss = summed[6]
    column_start = replica_rank * column_part
    table_old = lax.dynamic_slice_in_dim(embedding, column_start, column_part, 1).astype(
        jnp.float32
    )
    olds = [table_old] + [
        weight.astype(jnp.float32)
        for weight in (in_weight, out_weight, ahead_weight, conv_weight, head_params, norm_gains)
    ]
    element_counts = (
        VOCAB * D,
        D * IN_WIDTH,
        INNER * D,
        D * D,
        (KERNEL + 1) * CONV_WIDTH,
        3 * HEADS,
        GAINS,
    )
    row_counts = (VOCAB, D, INNER, D)
    row_olds = (table_rows, in_rows, out_rows, ahead_rows)
    column_olds = (table_columns, in_columns, out_columns, ahead_columns)
    squares = [gradient * gradient for gradient in gradients[:4]]
    table_rows_sum, table_weight = lax.psum(
        (jnp.sum(squares[0], axis=1), jnp.sum(table_old * table_old)), "dp"
    )
    own_rows = [table_rows_sum] + [jnp.sum(squares[position], axis=1) for position in range(1, 4)]
    own_totals = jnp.stack(
        [jnp.sum(row_sum) for row_sum in own_rows]
        + [jnp.sum(gradient * gradient) for gradient in gradients[4:]]
        + [table_weight]
        + [jnp.sum(weight * weight) for weight in olds[1:]]
        + [jnp.sum(row_state) for row_state in row_olds]
    )
    column_sums, totals = lax.psum(
        (tuple(jnp.sum(square, axis=0) for square in squares), own_totals), "fsdp"
    )
    weight_total = totals[7:14]
    grad_norm = jnp.sqrt(jnp.sum(totals[:7]))
    factor = jnp.minimum(1.0, CLIP_NORM / grad_norm)
    factor_squared = factor * factor
    clipped = [gradient * factor for gradient in gradients]
    column_counts = (D, IN_WIDTH, D, D)
    rows_new = [
        DECAY_RATE * row_olds[position]
        + (1.0 - DECAY_RATE) * factor_squared * own_rows[position] / column_counts[position]
        for position in range(4)
    ]
    columns_new = [
        DECAY_RATE * column_olds[position]
        + (1.0 - DECAY_RATE) * factor_squared * column_sums[position] / row_counts[position]
        for position in range(4)
    ]
    row_means = [
        (
            DECAY_RATE * totals[14 + position]
            + (1.0 - DECAY_RATE) * factor_squared * totals[position] / column_counts[position]
        )
        / row_counts[position]
        for position in range(4)
    ]
    step_sizes = [
        STEP_RATE
        * jnp.maximum(FLOOR_RMS, jnp.sqrt(weight_total[position] / element_counts[position]))
        for position in range(7)
    ]
    new_weights = []
    for position in range(4):
        estimate = (
            rows_new[position][:, None] * columns_new[position][None, :] / row_means[position]
        )
        new_weights.append(
            olds[position] - step_sizes[position] * clipped[position] * lax.rsqrt(estimate)
        )
    new_moments = []
    for position, old_moment in zip(range(4, 7), (conv_moment, head_moment, gain_moment)):
        moment_new = (
            DECAY_RATE * old_moment + (1.0 - DECAY_RATE) * clipped[position] * clipped[position]
        )
        new_moments.append(moment_new)
        new_weights.append(
            olds[position] - step_sizes[position] * clipped[position] * lax.rsqrt(moment_new)
        )
    return (
        new_weights[0],
        new_weights[1],
        new_weights[2],
        new_weights[3],
        new_weights[4],
        new_weights[5],
        new_weights[6],
        rows_new[0],
        columns_new[0],
        rows_new[1],
        columns_new[1],
        rows_new[2],
        columns_new[2],
        rows_new[3],
        columns_new[3],
        new_moments[0],
        new_moments[1],
        new_moments[2],
        loss,
        grad_norm,
    )


def solution(mesh):
    in_specs = (
        P(("dp", "fsdp")),
        P(("dp", "fsdp")),
        P(("dp", "fsdp"), None),
        P("fsdp", None),
        P("fsdp", None),
        P("fsdp", None),
        P("fsdp", None),
        P(None, "fsdp"),
        P(None, "fsdp"),
        P("fsdp"),
        P("fsdp"),
        P("dp"),
        P("fsdp"),
        P(),
        P("fsdp"),
        P(),
        P("fsdp"),
        P(),
        P(None, "fsdp"),
        P(None, "fsdp"),
        P("fsdp"),
    )
    out_specs = (
        P("fsdp", "dp"),
        P("fsdp", None),
        P("fsdp", None),
        P("fsdp", None),
        P(None, "fsdp"),
        P(None, "fsdp"),
        P("fsdp"),
        P("fsdp"),
        P("dp"),
        P("fsdp"),
        P(),
        P("fsdp"),
        P(),
        P("fsdp"),
        P(),
        P(None, "fsdp"),
        P(None, "fsdp"),
        P("fsdp"),
        P(),
        P(),
    )
    return jax.shard_map(shards, mesh=mesh, in_specs=in_specs, out_specs=out_specs, check_vma=False)
```

```python
import jax
import jax.numpy as jnp
from jax import lax
from jax.experimental import pallas as pl
from jax.experimental.pallas import tpu as pltpu
from jax.sharding import PartitionSpec as P

D = 1024
HEADS = 32
HEAD_DIM = 64
STATE = 128
VOCAB = 50688
KERNEL = 4
SPAN = 256
INNER = 2048
CONV_WIDTH = 2304
IN_WIDTH = 4384
GAINS = 4096
GROUP = 4
PAD = 8
CHUNK = 128
ROW_CHUNK = 512
TABLE_BLOCKS = 11
UNROLL = 8
ID_BITS = 14
TOK_DEV = 1024


PRECISE = lax.Precision.HIGHEST
EPSILON = 1e-05
DECAY_RATE = 0.5
STEP_RATE = 0.2
CLIP_NORM = 0.2
AFTER_SHARE = 0.3
FLOOR_RMS = 0.001
MASK_FILL = -10000.0


def merged_2(value, axis, join):
    pieces = jax.tree.map(lambda part: lax.all_gather(part, axis), value)
    head = jax.tree.map(lambda part: part[0], pieces)
    tail = jax.tree.map(lambda part: part[1:], pieces)
    running, _ = lax.scan(lambda running, piece: (join(running, piece), None), head, tail)
    return running


def rms_norm(values_in, gain_in):
    return (
        values_in
        * lax.rsqrt(jnp.mean(values_in * values_in, axis=-1, keepdims=True) + EPSILON)
        * gain_in
    )


def gated_norm(head_rows, gate_rows, gain_in):
    return rms_norm(head_rows * jax.nn.silu(gate_rows), gain_in)


def contract(one_side, other_side, one_dim, other_dim):
    return lax.dot_general(
        one_side,
        other_side,
        (((one_dim,), (other_dim,)), ((), ())),
        preferred_element_type=jnp.float32,
    )


def split(value):
    high = value.astype(jnp.bfloat16)
    return high, (value - high.astype(jnp.float32)).astype(jnp.bfloat16)


def product(one_side, other_side, one_dim, other_dim):
    return lax.dot_general(
        one_side,
        other_side,
        (((one_dim,), (other_dim,)), ((), ())),
        preferred_element_type=jnp.float32,
    )


def product_3(one_side, other_side, one_dim, other_dim):
    one_high, one_low = one_side
    other_high, other_low = other_side
    return (
        product(one_high, other_high, one_dim, other_dim)
        + product(one_low, other_high, one_dim, other_dim)
        + product(one_high, other_low, one_dim, other_dim)
    )


def exact(one_side, other_side, one_dim, other_dim):
    return lax.dot_general(
        one_side,
        other_side,
        (((one_dim,), (other_dim,)), ((), ())),
        precision=PRECISE,
        preferred_element_type=jnp.float32,
    )


def running_sum(values, backward):
    length = values.shape[1]
    lane = lax.broadcasted_iota(jnp.int32, values.shape, 1)
    shift = 1
    while shift < length:
        if backward:
            moved = pltpu.roll(values, length - shift, 1)
            values = values + jnp.where(lane < length - shift, moved, 0.0)
        else:
            moved = pltpu.roll(values, shift, 1)
            values = values + jnp.where(lane >= shift, moved, 0.0)
        shift *= 2
    return values


def taps_sum(window, taps_ref, rows):
    total = taps_ref[KERNEL : KERNEL + 1, :]
    for offset in range(KERNEL):
        start = PAD - KERNEL + 1 + offset
        total = total + taps_ref[offset : offset + 1, :] * window[start : start + rows]
    return total


def sigmoid(value):
    return 1.0 / (1.0 + jnp.exp(-value))


def decay_spread(row_decay, places, lane):
    here = lane == places
    at_place = jnp.sum(jnp.where(here, row_decay, 0.0), axis=1, keepdims=True)
    return jnp.exp(jnp.where(lane <= places, at_place - row_decay, MASK_FILL)), here


def mix_forward_kernel(
    normed_ref,
    weight_ref,
    taps_ref,
    raw_ref,
    columns_ref,
    places_ref,
    skip_ref,
    input_ref,
    out_ref,
    scores_ref,
    keys_ref,
    queries_ref,
    steps_ref,
    decay_ref,
    padded,
    active,
    mix_high,
    mix_low,
):
    step = pl.program_id(0)
    length = normed_ref.shape[0]
    rows = places_ref.shape[0]
    width = weight_ref.shape[1]
    chunk = CHUNK
    places = places_ref[...]
    lane = lax.broadcasted_iota(jnp.int32, (rows, length), 1)
    value = product(normed_ref[...], weight_ref[...], 1, 0)
    input_ref[...] = value
    padded[0:PAD, :] = jnp.zeros((PAD, width), jnp.float32)
    padded[PAD:, :] = value

    def activate(index, carry):
        start = pl.multiple_of(index * chunk, chunk)
        window = padded[pl.ds(start, chunk + PAD), :]
        total = taps_sum(window, taps_ref, chunk)
        active[pl.ds(start, chunk), :] = total * sigmoid(total)
        return carry

    lax.fori_loop(0, length // chunk, activate, 0)

    @pl.when(step == 0)
    def _():
        keys = active[:, :STATE]
        keys_ref[...] = keys
        picked = exact((lane == places).astype(jnp.float32), active[:, STATE:], 1, 0)
        queries_ref[...] = picked
        scores_ref[...] = exact(picked, keys, 1, 1)
        shifted = raw_ref[...] + columns_ref[:, 0:1]
        steps = jnp.maximum(shifted, 0.0) + jnp.log1p(jnp.exp(-jnp.abs(shifted)))
        steps_ref[...] = steps
        decay_ref[...] = running_sum(-steps * jnp.exp(columns_ref[:, 1:2]), False)

    @pl.when(step > 0)
    def _():
        scores = scores_ref[...]
        for index in range(GROUP):
            head = (step - 1) * GROUP + index
            row_steps = steps_ref[pl.ds(head, 1), :]
            spread, here = decay_spread(decay_ref[pl.ds(head, 1), :], places, lane)
            weights = scores * spread * row_steps + jnp.where(here, skip_ref[head], 0.0)
            high, low = split(weights)
            mix_high[index * rows : (index + 1) * rows, :] = high
            mix_low[index * rows : (index + 1) * rows, :] = low
        x_pair = split(active[...])
        mixed = product_3((mix_high[...], mix_low[...]), x_pair, 1, 0)
        column = lax.broadcasted_iota(jnp.int32, (rows, width), 1) // HEAD_DIM
        total = jnp.zeros((rows, width), jnp.float32)
        for index in range(GROUP):
            total = jnp.where(column == index, mixed[index * rows : (index + 1) * rows], total)
        out_ref[...] = total


def mix_forward(normed, weight, taps, raw, columns, places, skip):
    length = normed.shape[0]
    rows = places.shape[0]
    width = GROUP * HEAD_DIM
    blocks = CONV_WIDTH // width
    last = blocks - 1
    whole = lambda shape: pl.BlockSpec(shape, lambda step: (0,) * len(shape))
    turned = lambda step: (0, lax.rem(step + last, blocks))
    f32 = jnp.float32
    return pl.pallas_call(
        mix_forward_kernel,
        grid=(blocks,),
        in_specs=[
            whole((length, D)),
            pl.BlockSpec((D, width), turned),
            pl.BlockSpec((KERNEL + 1, width), turned),
            whole((HEADS, length)),
            whole((HEADS, 3)),
            whole((rows, 1)),
            pl.BlockSpec(memory_space=pltpu.SMEM),
        ],
        out_specs=[
            pl.BlockSpec((length, width), turned),
            pl.BlockSpec((rows, width), lambda step: (0, jnp.maximum(step - 1, 0))),
            whole((rows, length)),
            whole((length, STATE)),
            whole((rows, STATE)),
            whole((HEADS, length)),
            whole((HEADS, length)),
        ],
        out_shape=[
            jax.ShapeDtypeStruct((length, CONV_WIDTH), f32),
            jax.ShapeDtypeStruct((rows, INNER), f32),
            jax.ShapeDtypeStruct((rows, length), f32),
            jax.ShapeDtypeStruct((length, STATE), f32),
            jax.ShapeDtypeStruct((rows, STATE), f32),
            jax.ShapeDtypeStruct((HEADS, length), f32),
            jax.ShapeDtypeStruct((HEADS, length), f32),
        ],
        scratch_shapes=[
            pltpu.VMEM((length + PAD, width), f32),
            pltpu.VMEM((length, width), f32),
            pltpu.VMEM((GROUP * rows, length), jnp.bfloat16),
            pltpu.VMEM((GROUP * rows, length), jnp.bfloat16),
        ],
        compiler_params=pltpu.CompilerParams(vmem_limit_bytes=40 << 20),
        cost_estimate=pl.CostEstimate(
            flops=2 * length * D * CONV_WIDTH * 2,
            bytes_accessed=16 << 20,
            transcendentals=HEADS * rows * length,
        ),
        name="mix_forward",
    )(normed, weight, taps, raw, columns, places, skip)


def mix_backward_kernel(
    input_ref,
    taps_ref,
    grad_ref,
    scores_ref,
    keys_ref,
    queries_ref,
    steps_ref,
    decay_ref,
    raw_ref,
    columns_ref,
    places_ref,
    skip_ref,
    d_input_ref,
    d_taps_ref,
    d_raw_ref,
    d_columns_ref,
    padded,
    active,
    d_active,
    d_padded,
    mix_high,
    mix_low,
    d_mix,
    d_scores,
    d_steps,
    from_place,
    d_skip,
):
    step = pl.program_id(0)
    last = pl.num_programs(0) - 1
    length, width = input_ref.shape
    rows = places_ref.shape[0]
    chunk = CHUNK
    count = length // chunk
    places = places_ref[...]
    lane = lax.broadcasted_iota(jnp.int32, (rows, length), 1)
    padded[0:PAD, :] = jnp.zeros((PAD, width), jnp.float32)
    padded[PAD:, :] = input_ref[...]

    @pl.when(step == 0)
    def _():
        d_scores[...] = jnp.zeros_like(d_scores)

    @pl.when(step < last)
    def _():
        def activate(index, carry):
            start = pl.multiple_of(index * chunk, chunk)
            window = padded[pl.ds(start, chunk + PAD), :]
            total = taps_sum(window, taps_ref, chunk)
            active[pl.ds(start, chunk), :] = total * sigmoid(total)
            return carry

        lax.fori_loop(0, count, activate, 0)
        x_pair = split(active[...])
        column = lax.broadcasted_iota(jnp.int32, (rows, width), 1) // HEAD_DIM
        grad = grad_ref[...]
        stacked = split(
            jnp.concatenate(
                [jnp.where(column == index, grad, 0.0) for index in range(GROUP)], axis=0
            )
        )
        d_mix[...] = product_3(stacked, x_pair, 1, 1)
        scores = scores_ref[...]
        for index in range(GROUP):
            head = step * GROUP + index
            row_steps = steps_ref[pl.ds(head, 1), :]
            spread, here = decay_spread(decay_ref[pl.ds(head, 1), :], places, lane)
            weights = scores * spread
            part = d_mix[index * rows : (index + 1) * rows, :]
            d_scores[...] += part * spread * row_steps
            shared = part * weights
            d_steps[pl.ds(head, 1), :] = jnp.sum(shared, axis=0, keepdims=True)
            row_total = jnp.sum(shared * row_steps, axis=1, keepdims=True)
            from_place[pl.ds(head, 1), :] = jnp.sum(
                jnp.where(lane <= places, row_total, 0.0), axis=0, keepdims=True
            )
            d_skip[pl.ds(head, 1), :] = jnp.sum(
                jnp.where(here, part, 0.0), axis=0, keepdims=True
            )
            full = weights * row_steps + jnp.where(here, skip_ref[head], 0.0)
            high, low = split(full)
            mix_high[index * rows : (index + 1) * rows, :] = high
            mix_low[index * rows : (index + 1) * rows, :] = low
        d_active[...] = product_3((mix_high[...], mix_low[...]), stacked, 0, 0)

    @pl.when(step == last)
    def _():
        onehot = (lane == places).astype(jnp.float32)
        d_score = d_scores[...]
        d_queries = exact(d_score, keys_ref[...], 1, 0)
        d_active[:, :STATE] = exact(d_score, queries_ref[...], 0, 0)
        d_active[:, STATE:] = exact(onehot, d_queries, 0, 0)
        steps = steps_ref[...]
        direct = d_steps[...]
        rates_scale = -jnp.exp(columns_ref[:, 1:2])
        d_rates = from_place[...] - running_sum(direct * steps, True)
        d_step = direct + d_rates * rates_scale
        d_raw = d_step * sigmoid(raw_ref[...] + columns_ref[:, 0:1])
        d_raw_ref[...] = d_raw
        d_log = jnp.sum(d_rates * steps, axis=1, keepdims=True) * rates_scale
        slot = lax.broadcasted_iota(jnp.int32, d_columns_ref.shape, 1)
        d_columns_ref[...] = jnp.where(
            slot == 0,
            jnp.sum(d_raw, axis=1, keepdims=True),
            jnp.where(slot == 1, d_log, jnp.sum(d_skip[...], axis=1, keepdims=True)),
        )

    d_padded[length:, :] = jnp.zeros((PAD, width), jnp.float32)

    def through_silu(index, carry):
        start = pl.multiple_of(index * chunk, chunk)
        window = padded[pl.ds(start, chunk + PAD), :]
        total = taps_sum(window, taps_ref, chunk)
        gate = sigmoid(total)
        d_total = d_active[pl.ds(start, chunk), :] * (gate * (1.0 + total * (1.0 - gate)))
        d_padded[pl.ds(start, chunk), :] = d_total
        sums = []
        for offset in range(KERNEL):
            begin = PAD - KERNEL + 1 + offset
            sums.append(jnp.sum(d_total * window[begin : begin + chunk], axis=0, keepdims=True))
        sums.append(jnp.sum(d_total, axis=0, keepdims=True))
        return tuple(one + other for one, other in zip(carry, sums))

    sums = lax.fori_loop(
        0, count, through_silu, tuple(jnp.zeros((1, width), jnp.float32) for _ in range(KERNEL + 1))
    )
    for offset in range(KERNEL + 1):
        d_taps_ref[offset : offset + 1, :] = sums[offset]

    def through_taps(index, carry):
        start = pl.multiple_of(index * chunk, chunk)
        window = d_padded[pl.ds(start, chunk + PAD), :]
        total = taps_ref[KERNEL - 1 : KERNEL, :] * window[:chunk]
        for offset in range(KERNEL - 1):
            begin = KERNEL - 1 - offset
            total = total + taps_ref[offset : offset + 1, :] * window[begin : begin + chunk]
        d_input_ref[pl.ds(start, chunk), :] = total.astype(d_input_ref.dtype)
        return carry

    lax.fori_loop(0, count, through_taps, 0)


def mix_backward(inputs, taps, grad, scores, keys, queries, steps, decay, raw, columns, places, skip):
    length = inputs.shape[0]
    rows = places.shape[0]
    width = GROUP * HEAD_DIM
    blocks = CONV_WIDTH // width
    whole = lambda shape: pl.BlockSpec(shape, lambda step: (0,) * len(shape))
    along = lambda step: (0, step)
    f32 = jnp.float32
    return pl.pallas_call(
        mix_backward_kernel,
        grid=(blocks,),
        in_specs=[
            pl.BlockSpec((length, width), along),
            pl.BlockSpec((KERNEL + 1, width), along),
            pl.BlockSpec((rows, width), lambda step: (0, jnp.minimum(step, blocks - 2))),
            whole((rows, length)),
            whole((length, STATE)),
            whole((rows, STATE)),
            whole((HEADS, length)),
            whole((HEADS, length)),
            whole((HEADS, length)),
            whole((HEADS, 3)),
            whole((rows, 1)),
            pl.BlockSpec(memory_space=pltpu.SMEM),
        ],
        out_specs=[
            pl.BlockSpec((length, width), along),
            pl.BlockSpec((KERNEL + 1, width), along),
            whole((HEADS, length)),
            whole((HEADS, 128)),
        ],
        out_shape=[
            jax.ShapeDtypeStruct((length, CONV_WIDTH), jnp.bfloat16),
            jax.ShapeDtypeStruct((KERNEL + 1, CONV_WIDTH), f32),
            jax.ShapeDtypeStruct((HEADS, length), f32),
            jax.ShapeDtypeStruct((HEADS, 128), f32),
        ],
        scratch_shapes=[
            pltpu.VMEM((length + PAD, width), f32),
            pltpu.VMEM((length, width), f32),
            pltpu.VMEM((length, width), f32),
            pltpu.VMEM((length + PAD, width), f32),
            pltpu.VMEM((GROUP * rows, length), jnp.bfloat16),
            pltpu.VMEM((GROUP * rows, length), jnp.bfloat16),
            pltpu.VMEM((GROUP * rows, length), f32),
            pltpu.VMEM((rows, length), f32),
            pltpu.VMEM((HEADS, length), f32),
            pltpu.VMEM((HEADS, length), f32),
            pltpu.VMEM((HEADS, length), f32),
        ],
        compiler_params=pltpu.CompilerParams(vmem_limit_bytes=48 << 20),
        cost_estimate=pl.CostEstimate(
            flops=6 * HEADS * rows * length * HEAD_DIM * 4,
            bytes_accessed=20 << 20,
            transcendentals=HEADS * rows * length,
        ),
        name="mix_backward",
    )(inputs, taps, grad, scores, keys, queries, steps, decay, raw, columns, places, skip)


def table_kernel(
    first_id_ref,
    table_ref,
    rows_ref,
    columns_ref,
    marks_ref,
    own_ref,
    other_ref,
):
    block = table_ref.shape[0]
    width = own_ref.shape[1]
    count = rows_ref.shape[0] // ROW_CHUNK
    entries = (
        first_id_ref[0]
        + pl.program_id(0) * block
        + lax.broadcasted_iota(jnp.int32, (block, ROW_CHUNK), 0)
    )
    table = table_ref[...]

    def part(start):
        logits = product(table, rows_ref[pl.ds(start, ROW_CHUNK), :], 1, 1)
        marks = marks_ref[:, pl.ds(start, ROW_CHUNK)]
        share = jnp.exp(logits - marks[0:1])
        share = jnp.where(entries == marks[1:2].astype(jnp.int32), share - 1.0, share)
        grad = (share * marks[2:3]).astype(jnp.bfloat16)
        return product(grad, columns_ref[pl.ds(start, ROW_CHUNK), :], 1, 0)

    def body(index, total):
        start = pl.multiple_of(index * 2 * ROW_CHUNK, 2 * ROW_CHUNK)
        return total + (part(start) + part(start + ROW_CHUNK))

    total = lax.fori_loop(0, count // 2, body, jnp.zeros((block, 2 * width), jnp.float32))
    own_ref[...] = total[:, :width]
    other_ref[...] = total[:, width:].astype(other_ref.dtype)


def table_grads(first_id, table, rows, columns, marks):
    vocab_part = table.shape[0]
    width = columns.shape[1] // 2
    block = vocab_part // TABLE_BLOCKS
    once = lambda shape: pl.BlockSpec(
        shape, lambda step: (0,) * len(shape), pipeline_mode=pl.Buffered(1)
    )
    return pl.pallas_call(
        table_kernel,
        grid=(TABLE_BLOCKS,),
        in_specs=[
            pl.BlockSpec(memory_space=pltpu.SMEM),
            pl.BlockSpec((block, D), lambda step: (step, 0)),
            once(rows.shape),
            once(columns.shape),
            once(marks.shape),
        ],
        out_specs=[
            pl.BlockSpec((block, width), lambda step: (step, 0)),
            pl.BlockSpec((block, width), lambda step: (step, 0)),
        ],
        out_shape=[
            jax.ShapeDtypeStruct((vocab_part, width), jnp.float32),
            jax.ShapeDtypeStruct((vocab_part, width), jnp.bfloat16),
        ],
        compiler_params=pltpu.CompilerParams(vmem_limit_bytes=56 << 20),
        cost_estimate=pl.CostEstimate(
            flops=2 * vocab_part * rows.shape[0] * (D + 2 * width),
            bytes_accessed=2 * vocab_part * D + 6 * vocab_part * width,
            transcendentals=vocab_part * rows.shape[0],
        ),
        name="table_grads",
    )(first_id, table, rows, columns, marks)


def token_kernel(
    counts_ref,
    listing_ref,
    grads_ref,
    own_ref,
    other_ref,
    out_ref,
    held,
    second,
    third,
    fourth,
):
    step = pl.program_id(0)
    length = grads_ref.shape[1]
    totals = (out_ref, second, third, fourth)

    @pl.when(step == 0)
    def _():
        out_ref[...] = own_ref[...] + other_ref[...].astype(jnp.float32)
        for total in totals[1:]:
            total[...] = jnp.zeros_like(total)
        held[length:, :] = jnp.zeros((PAD, held.shape[1]), jnp.float32)

    held[0:length, :] = grads_ref[0].astype(jnp.float32)

    def body(index, carry):
        for offset in range(UNROLL):
            entry = listing_ref[0, 0, index * UNROLL + offset]
            source = lax.shift_right_logical(entry, ID_BITS) & (2 * TOK_DEV - 1)
            target = entry & ((1 << ID_BITS) - 1)
            total = totals[offset % len(totals)]
            total[pl.ds(target, 1), :] += held[pl.ds(source, 1), :]
        return carry

    lax.fori_loop(0, (counts_ref[step] + UNROLL - 1) // UNROLL, body, 0)

    @pl.when(step == pl.num_programs(0) - 1)
    def _():
        out_ref[...] += second[...] + (third[...] + fourth[...])


def token_grads(counts, listing, grads, own, other):
    sources, length, width = grads.shape
    once = lambda shape: pl.BlockSpec(
        shape, lambda step: (0,) * len(shape), pipeline_mode=pl.Buffered(1)
    )
    return pl.pallas_call(
        token_kernel,
        grid=(sources,),
        in_specs=[
            pl.BlockSpec(memory_space=pltpu.SMEM),
            pl.BlockSpec((1, 1, length), lambda step: (step, 0, 0), memory_space=pltpu.SMEM),
            pl.BlockSpec((1, length, width), lambda step: (step, 0, 0)),
            once(own.shape),
            once(other.shape),
        ],
        out_specs=pl.BlockSpec(own.shape, lambda step: (0, 0)),
        out_shape=jax.ShapeDtypeStruct(own.shape, jnp.float32),
        scratch_shapes=[pltpu.VMEM((length + PAD, width), jnp.float32)]
        + [pltpu.VMEM(own.shape, jnp.float32)] * 3,
        compiler_params=pltpu.CompilerParams(vmem_limit_bytes=56 << 20),
        cost_estimate=pl.CostEstimate(
            flops=sources * length * width,
            bytes_accessed=64 << 20,
            transcendentals=0,
        ),
        name="token_grads",
    )(counts, listing, grads, own, other)


def shard_terms(logits, local_target):
    row_max = jnp.max(logits, axis=1)
    exp_total = jnp.sum(jnp.exp(logits - row_max[:, None]), axis=1)
    onehot = (jnp.arange(logits.shape[1])[None, :] == local_target[:, None]).astype(jnp.float32)
    picked = jnp.sum(onehot * logits, axis=1)
    return (row_max, exp_total, picked, onehot)


def combine_totals(one_side, other_side):
    combined = []
    for base in (0, 3):
        row_max = jnp.maximum(one_side[base], other_side[base])
        exp_total = one_side[base + 1] * jnp.exp(one_side[base] - row_max) + other_side[
            base + 1
        ] * jnp.exp(other_side[base] - row_max)
        combined = combined + [row_max, exp_total, one_side[base + 2] + other_side[base + 2]]
    return tuple(combined)


def shards(
    tokens,
    lengths,
    loss_picks,
    embedding,
    in_weight,
    out_weight,
    ahead_weight,
    conv_weight,
    head_params,
    norm_gains,
    table_rows,
    table_columns,
    in_rows,
    in_columns,
    out_rows,
    out_columns,
    ahead_rows,
    ahead_columns,
    conv_moment,
    head_moment,
    gain_moment,
):
    group_size = lax.axis_size("fsdp")
    my_rank = lax.axis_index("fsdp")
    replica_count = lax.axis_size("dp")
    replica_rank = lax.axis_index("dp")
    seq_len = tokens.shape[0]
    places = loss_picks[0] % (lengths[0] - 2)
    loss_rows = places.shape[0]
    packed = jnp.concatenate([tokens, tokens[places + 1], tokens[places + 2]])
    group_ids = lax.all_gather(packed, "fsdp", axis=0, tiled=True).reshape(
        group_size, seq_len + 2 * loss_rows
    )
    all_tokens = group_ids[:, :seq_len].reshape(-1)
    next_ids = group_ids[:, seq_len : seq_len + loss_rows].reshape(-1)
    after_ids = group_ids[:, seq_len + loss_rows :].reshape(-1)
    vocab_part = embedding.shape[0]
    width_total = embedding.shape[1]
    column_part = width_total // replica_count
    first_id = my_rank * vocab_part
    local_ids = all_tokens - first_id
    inside = (local_ids >= 0) & (local_ids < vocab_part)
    safe_ids = jnp.clip(local_ids, 0, vocab_part - 1)
    every_token = lax.all_gather(tokens, ("fsdp", "dp"), axis=0)
    every_id = every_token - first_id
    every_inside = (every_id >= 0) & (every_id < vocab_part)
    slot = jnp.arange(seq_len, dtype=jnp.int32)[None, :]
    listing = lax.sort(
        jnp.where(every_inside, (slot << ID_BITS) + every_id, (2 * seq_len - 1) * (1 << ID_BITS)),
        dimension=1,
        is_stable=False,
    )
    listing = jnp.where(listing < (seq_len << ID_BITS), listing, seq_len << ID_BITS)
    inside_counts = jnp.sum(every_inside.astype(jnp.int32), axis=1)
    looked = jnp.where(inside[:, None], embedding[safe_ids], jnp.zeros((), jnp.bfloat16)).astype(
        jnp.float32
    )
    embedded = lax.psum_scatter(
        looked.astype(jnp.bfloat16), "fsdp", scatter_dimension=0, tiled=True
    ).astype(jnp.float32)
    in_gate, in_conv, in_step, out_matrix, ahead_matrix, conv_table, head_table, gain_table = (
        lax.all_gather(in_weight[:, :INNER], "fsdp", axis=0, tiled=True),
        lax.all_gather(in_weight[:, INNER : INNER + CONV_WIDTH], "fsdp", axis=0, tiled=True),
        lax.all_gather(in_weight[:, INNER + CONV_WIDTH :], "fsdp", axis=0, tiled=True),
        lax.all_gather(out_weight, "fsdp", axis=0, tiled=True),
        lax.all_gather(ahead_weight, "fsdp", axis=0, tiled=True),
        lax.all_gather(conv_weight, "fsdp", axis=1, tiled=True).astype(jnp.float32),
        lax.all_gather(head_params, "fsdp", axis=1, tiled=True).astype(jnp.float32),
        lax.all_gather(norm_gains, "fsdp", axis=0, tiled=True).astype(jnp.float32),
    )
    normed, pull_pre = jax.vjp(rms_norm, embedded, gain_table[:D])
    normed_low = normed.astype(jnp.bfloat16)
    raw = contract(in_step, normed_low, 0, 1)
    columns = head_table.T
    place_column = places[:, None]
    inputs, head_rows, scores, keys, queries, steps, decay = mix_forward(
        normed_low, in_conv, conv_table, raw, columns, place_column, head_table[2]
    )
    embedded_rows = embedded[places]
    normed_rows, pull_rows = jax.vjp(rms_norm, embedded_rows, gain_table[:D])
    normed_rows = normed_rows.astype(jnp.bfloat16)
    gate_rows = contract(normed_rows, in_gate, 1, 0)
    mixed, pull_mix = jax.vjp(gated_norm, head_rows, gate_rows, gain_table[D + D :])
    mixed_low = mixed.astype(jnp.bfloat16)
    residual = embedded_rows + contract(mixed_low, out_matrix, 1, 0)
    final_norm, pull_final = jax.vjp(rms_norm, residual, gain_table[D : D + D])
    first_low = final_norm.astype(jnp.bfloat16)
    second_low = jnp.dot(first_low, ahead_matrix, preferred_element_type=jnp.float32).astype(
        jnp.bfloat16
    )
    group_first, group_second = (
        lax.all_gather(first_low, "fsdp", axis=0, tiled=True),
        lax.all_gather(second_low, "fsdp", axis=0, tiled=True),
    )
    logits_next = contract(group_first, embedding, 1, 1)
    logits_after = contract(group_second, embedding, 1, 1)
    max_next, sum_next, pick_next, hot_next = shard_terms(logits_next, next_ids - first_id)
    max_after, sum_after, pick_after, hot_after = shard_terms(logits_after, after_ids - first_id)
    merged = merged_2(
        (max_next, sum_next, pick_next, max_after, sum_after, pick_after), "fsdp", combine_totals
    )
    lse_next = merged[0] + jnp.log(merged[1])
    lse_after = merged[3] + jnp.log(merged[4])
    count_all = loss_rows * group_size * replica_count
    group_loss = (
        jnp.sum(lse_next - merged[2]) + AFTER_SHARE * jnp.sum(lse_after - merged[5])
    ) / count_all
    grad_next = ((jnp.exp(logits_next - lse_next[:, None]) - hot_next) / count_all).astype(
        jnp.bfloat16
    )
    grad_after = (
        (jnp.exp(logits_after - lse_after[:, None]) - hot_after) * (AFTER_SHARE / count_all)
    ).astype(jnp.bfloat16)
    rows_next_grad = contract(grad_next, embedding, 1, 0)
    rows_after_grad = contract(grad_after, embedding, 1, 0)
    d_first_own, d_second_own = (
        lax.psum_scatter(rows_next_grad, "fsdp", scatter_dimension=0, tiled=True),
        lax.psum_scatter(rows_after_grad, "fsdp", scatter_dimension=0, tiled=True),
    )
    d_second = d_second_own.astype(jnp.bfloat16)
    d_ahead = contract(first_low, d_second, 0, 0)
    d_first = d_first_own + contract(d_second, ahead_matrix, 1, 1)
    d_residual, d_gain_final = pull_final(d_first)
    d_out = d_residual.astype(jnp.bfloat16)
    d_out_weight = contract(mixed_low, d_out, 0, 0)
    d_mixed = contract(d_out, out_matrix, 1, 1)
    d_head_rows, d_gate, d_gain_mix = pull_mix(d_mixed)
    d_gate_low = d_gate.astype(jnp.bfloat16)
    d_in_gate = contract(normed_rows, d_gate_low, 0, 0)
    d_pre_rows, d_gain_rows = pull_rows(contract(d_gate_low, in_gate, 1, 1))
    d_inputs, d_conv, d_raw, d_columns = mix_backward(
        inputs,
        conv_table,
        d_head_rows,
        scores,
        keys,
        queries,
        steps,
        decay,
        raw,
        columns,
        place_column,
        head_table[2],
    )
    d_heads = d_columns[:, :3].T
    d_raw_low = d_raw.astype(jnp.bfloat16)
    d_in_conv = contract(normed_low, d_inputs, 0, 0)
    d_in_step = contract(normed_low, d_raw_low, 0, 1)
    d_normed = contract(d_inputs, in_conv, 1, 1) + contract(d_raw_low, in_step, 0, 1)
    d_pre, d_gain_first = pull_pre(d_normed)
    d_gain_first = d_gain_first + d_gain_rows
    onehot = (lax.broadcasted_iota(jnp.int32, (seq_len, loss_rows), 0) == places[None, :]).astype(
        jnp.float32
    )
    d_embedded = d_pre + jnp.dot(onehot, d_residual + d_pre_rows, precision=PRECISE)
    d_gains = jnp.concatenate([d_gain_first, d_gain_final, d_gain_mix])
    low_shares = tuple(
        lax.psum_scatter(gradient.astype(jnp.bfloat16), "fsdp", scatter_dimension=0, tiled=True)
        for gradient in (d_in_conv, d_in_gate, d_out_weight, d_ahead)
    )
    shares = (
        lax.psum_scatter(d_in_step, "fsdp", scatter_dimension=0, tiled=True),
        lax.psum_scatter(d_conv, "fsdp", scatter_dimension=1, tiled=True),
        lax.psum_scatter(d_heads, "fsdp", scatter_dimension=1, tiled=True),
        lax.psum_scatter(d_gains, "fsdp", scatter_dimension=0, tiled=True),
    )
    column_start = replica_rank * column_part
    other_start = (replica_rank ^ 1) * column_part
    peers = [list(range(parity, replica_count, 2)) for parity in range(2)]
    pair_rows = lax.all_gather(
        jnp.concatenate([group_first, group_second]), "dp", axis=0, tiled=True, axis_index_groups=peers
    )
    pair_marks = lax.all_gather(
        jnp.stack(
            [
                jnp.concatenate([lse_next, lse_after]),
                jnp.concatenate([next_ids, after_ids]).astype(jnp.float32),
            ]
        ),
        "dp",
        axis=1,
        tiled=True,
        axis_index_groups=peers,
    )
    row_shares = jnp.where(
        jnp.arange(pair_rows.shape[0]) % (2 * group_size * loss_rows) < group_size * loss_rows,
        1.0 / count_all,
        AFTER_SHARE / count_all,
    ).astype(jnp.float32)
    own_table, other_table = table_grads(
        jnp.reshape(first_id, (1,)).astype(jnp.int32),
        embedding,
        pair_rows,
        jnp.concatenate(
            [
                lax.dynamic_slice_in_dim(pair_rows, column_start, column_part, 1),
                lax.dynamic_slice_in_dim(pair_rows, other_start, column_part, 1),
            ],
            axis=1,
        ),
        jnp.concatenate([pair_marks, row_shares[None, :]]),
    )
    other_table = lax.ppermute(
        other_table, "dp", [(index, index ^ 1) for index in range(replica_count)]
    )
    column_grads = lax.all_to_all(
        d_embedded.astype(jnp.bfloat16).reshape(seq_len, replica_count, column_part),
        "dp",
        split_axis=1,
        concat_axis=0,
    )
    column_grads = lax.all_gather(column_grads, "fsdp", axis=0, tiled=True)
    table_own = token_grads(
        inside_counts, listing[:, None, :], column_grads, own_table, other_table
    )
    low_sums = [total.astype(jnp.float32) for total in lax.psum(low_shares, "dp")]
    sums = lax.psum((shares, group_loss), "dp")
    loss = sums[1]
    gradients = [
        table_own,
        jnp.concatenate([low_sums[1], low_sums[0], sums[0][0]], axis=1),
        low_sums[2],
        low_sums[3],
    ] + list(sums[0][1:])
    table_old = lax.dynamic_slice_in_dim(embedding, column_start, column_part, 1).astype(
        jnp.float32
    )
    olds = [table_old] + [
        weight.astype(jnp.float32)
        for weight in (in_weight, out_weight, ahead_weight, conv_weight, head_params, norm_gains)
    ]
    element_counts = (
        VOCAB * D,
        D * IN_WIDTH,
        INNER * D,
        D * D,
        (KERNEL + 1) * CONV_WIDTH,
        3 * HEADS,
        GAINS,
    )
    row_counts = (VOCAB, D, INNER, D)
    row_olds = (table_rows, in_rows, out_rows, ahead_rows)
    column_olds = (table_columns, in_columns, out_columns, ahead_columns)
    squares = [gradient * gradient for gradient in gradients[:4]]
    table_rows_sum, table_weight = lax.psum(
        (jnp.sum(squares[0], axis=1), jnp.sum(table_old * table_old)), "dp"
    )
    own_rows = [table_rows_sum] + [jnp.sum(squares[position], axis=1) for position in range(1, 4)]
    own_totals = jnp.stack(
        [jnp.sum(row_sum) for row_sum in own_rows]
        + [jnp.sum(gradient * gradient) for gradient in gradients[4:]]
        + [table_weight]
        + [jnp.sum(weight * weight) for weight in olds[1:]]
        + [jnp.sum(row_state) for row_state in row_olds]
    )
    column_sums, totals = lax.psum(
        (tuple(jnp.sum(square, axis=0) for square in squares), own_totals), "fsdp"
    )
    weight_total = totals[7:14]
    grad_norm = jnp.sqrt(jnp.sum(totals[:7]))
    factor = jnp.minimum(1.0, CLIP_NORM / grad_norm)
    factor_squared = factor * factor
    clipped = [gradient * factor for gradient in gradients]
    column_counts = (D, IN_WIDTH, D, D)
    rows_new = [
        DECAY_RATE * row_olds[position]
        + (1.0 - DECAY_RATE) * factor_squared * own_rows[position] / column_counts[position]
        for position in range(4)
    ]
    columns_new = [
        DECAY_RATE * column_olds[position]
        + (1.0 - DECAY_RATE) * factor_squared * column_sums[position] / row_counts[position]
        for position in range(4)
    ]
    row_means = [
        (
            DECAY_RATE * totals[14 + position]
            + (1.0 - DECAY_RATE) * factor_squared * totals[position] / column_counts[position]
        )
        / row_counts[position]
        for position in range(4)
    ]
    step_sizes = [
        STEP_RATE
        * jnp.maximum(FLOOR_RMS, jnp.sqrt(weight_total[position] / element_counts[position]))
        for position in range(7)
    ]
    new_weights = []
    for position in range(4):
        estimate = (
            rows_new[position][:, None] * columns_new[position][None, :] / row_means[position]
        )
        new_weights.append(
            olds[position] - step_sizes[position] * clipped[position] * lax.rsqrt(estimate)
        )
    new_moments = []
    for position, old_moment in zip(range(4, 7), (conv_moment, head_moment, gain_moment)):
        moment_new = (
            DECAY_RATE * old_moment + (1.0 - DECAY_RATE) * clipped[position] * clipped[position]
        )
        new_moments.append(moment_new)
        new_weights.append(
            olds[position] - step_sizes[position] * clipped[position] * lax.rsqrt(moment_new)
        )
    return (
        new_weights[0],
        new_weights[1],
        new_weights[2],
        new_weights[3],
        new_weights[4],
        new_weights[5],
        new_weights[6],
        rows_new[0],
        columns_new[0],
        rows_new[1],
        columns_new[1],
        rows_new[2],
        columns_new[2],
        rows_new[3],
        columns_new[3],
        new_moments[0],
        new_moments[1],
        new_moments[2],
        loss,
        grad_norm,
    )


def solution(mesh):
    in_specs = (
        P(("dp", "fsdp")),
        P(("dp", "fsdp")),
        P(("dp", "fsdp"), None),
        P("fsdp", None),
        P("fsdp", None),
        P("fsdp", None),
        P("fsdp", None),
        P(None, "fsdp"),
        P(None, "fsdp"),
        P("fsdp"),
        P("fsdp"),
        P("dp"),
        P("fsdp"),
        P(),
        P("fsdp"),
        P(),
        P("fsdp"),
        P(),
        P(None, "fsdp"),
        P(None, "fsdp"),
        P("fsdp"),
    )
    out_specs = (
        P("fsdp", "dp"),
        P("fsdp", None),
        P("fsdp", None),
        P("fsdp", None),
        P(None, "fsdp"),
        P(None, "fsdp"),
        P("fsdp"),
        P("fsdp"),
        P("dp"),
        P("fsdp"),
        P(),
        P("fsdp"),
        P(),
        P("fsdp"),
        P(),
        P(None, "fsdp"),
        P(None, "fsdp"),
        P("fsdp"),
        P(),
        P(),
    )
    return jax.shard_map(shards, mesh=mesh, in_specs=in_specs, out_specs=out_specs, check_vma=False)
```
